32 devices in a mesh: dp: 2 (over z, core), tp: 16 (over x, y).
Axes of the slice: x: 4, y: 4, z: 1, core: 2. Of those that a mesh axis runs over, the one named last changes fastest.
The devices are a block of a 4x4x8 slice.
Arguments:
- x: bfloat16 [4096, 8192], P('dp'), parts along dimension 0
- w_gate: bfloat16 [8192, 49152], P(None, 'tp')
- w_up: bfloat16 [8192, 49152], P(None, 'tp')
- w_down: bfloat16 [49152, 8192], P('tp')
Outputs:
- output: bfloat16 [4096, 8192], P('dp'), parts along dimension 0
There are 2 independent parts. The reference program is written for one: setup_inputs(seed, part) draws one part's arguments, and reference() takes and returns one part's arrays. A program takes and returns all parts, laid end to end along the dimension named above; an argument that names none is the same for every part.
All inputs are finite; a program needn't handle non-finite values.
Results may differ from the reference program's by a relative error of at most 0.016.
Values are sent between devices in bfloat16 or wider.
A program may use at most 768 MiB of HBM per device.

```python
import jax
import jax.numpy as jnp

ROWS = 2048
D = 8192
FF = 49152


def setup_inputs(seed: int = 0, part: int = 0) -> dict:
    kx, kg, ku, kd = jax.random.split(jax.random.key(seed), 4)
    drawn = {
        "x": jax.random.normal(jax.random.fold_in(kx, part), (ROWS, D), jnp.float32),
        "w_gate": jax.random.normal(kg, (D, FF), jnp.float32) * D**-0.5,
        "w_up": jax.random.normal(ku, (D, FF), jnp.float32) * D**-0.5,
        "w_down": jax.random.normal(kd, (FF, D), jnp.float32) * FF**-0.5,
    }
    return {k: v.astype(jnp.bfloat16) for k, v in drawn.items()}


def reference(x, w_gate, w_up, w_down):
    gate = jnp.dot(x, w_gate, preferred_element_type=jnp.float32)
    up = jnp.dot(x, w_up, preferred_element_type=jnp.float32)
    hidden = (jax.nn.silu(gate) * up).astype(jnp.bfloat16)
    return jnp.dot(hidden, w_down, preferred_element_type=jnp.float32).astype(jnp.bfloat16)
```

```python
import functools
import math

import jax
import jax.numpy as jnp
from jax import lax
from jax.experimental import pallas as pl
from jax.experimental.pallas import tpu as pltpu
from jax.sharding import PartitionSpec as P

MESH = pl.DeviceIdType.MESH
CHUNK = 512
GATE_TICKS = 12
STEPS = 6
STREAMS = ((0, 1), (0, -1), (1, 1), (1, -1))


def kernel(side, chunk, x_hbm, wg_hbm, wu_hbm, wd_hbm, y_hbm,
           x_v, h_v, wg_v, wu_v, wd_v, t_v, r1, s1, r2, s2,
           x_sem, wg_sem, wu_sem, wd_sem,
           r1_sem, s1_sem, r2_sem, s2_sem, g2_recv, g2_send, g1_recv, g1_send, own_sem,
           free1, free2):
    rows = x_hbm.shape[0]
    nk = rows // chunk
    rb = chunk // 2
    rs = rb // side
    tn = wg_v.shape[2]
    ct = wd_v.shape[2]
    gate_ticks = wg_hbm.shape[1] // tn
    down_ticks = 4 * side
    ticks = gate_ticks + down_ticks
    me = lax.axis_index("tp")
    pos = (me // side, me % side)

    def device(axis, shift):
        p0, p1 = pos
        if axis == 0:
            p0 = (p0 + shift + side) % side
        else:
            p1 = (p1 + shift + side) % side
        return {"tp": p0 * side + p1}

    barrier = pltpu.get_barrier_semaphore()
    for axis, shift in STREAMS:
        pl.semaphore_signal(barrier, inc=1, device_id=device(axis, shift), device_id_type=MESH)
    pl.semaphore_wait(barrier, 4)

    def x_copy(k):
        return pltpu.make_async_copy(x_hbm.at[pl.ds(k * chunk, chunk), :], x_v, x_sem)

    def gate_copies(j):
        cols = pl.ds(pl.multiple_of(j * tn, tn), tn)
        s = j % 2
        return (
            pltpu.make_async_copy(wg_hbm.at[:, cols], wg_v.at[s], wg_sem.at[s]),
            pltpu.make_async_copy(wu_hbm.at[:, cols], wu_v.at[s], wu_sem.at[s]),
        )

    def down_copy(q):
        c, step = q % 4, q // 4
        along = jnp.where(c < 2, pos[0], pos[1])
        way = 1 - 2 * (c % 2)
        piece = (along - way * (1 + step) + 2 * side) % side
        cols = pl.ds(pl.multiple_of((c * side + piece) * ct, ct), ct)
        s = q % 2
        return pltpu.make_async_copy(wd_hbm.at[:, cols], wd_v.at[s], wd_sem.at[s])

    def piece1(c, e):
        axis, way = STREAMS[c]
        return (pos[axis] - way * (1 + e) + 3 * side) % side

    def piece2(c, e):
        axis, way = STREAMS[c]
        return (pos[1 - axis] - way * (1 + e) + 3 * side) % side

    def to1(c):
        axis, way = STREAMS[c]
        return device(axis, way)

    def from1(c):
        axis, way = STREAMS[c]
        return device(axis, -way)

    def to2(c):
        axis, way = STREAMS[c]
        return device(1 - axis, way)

    def from2(c):
        axis, way = STREAMS[c]
        return device(1 - axis, -way)

    def rs1_copy(k, b, c, hop):
        slot = ((side - 1) * k + hop) % 2
        return pltpu.make_async_remote_copy(
            src_ref=s1.at[b, c], dst_ref=r1.at[b, c, slot],
            send_sem=s1_sem.at[b, c], recv_sem=r1_sem.at[b, c, slot],
            device_id=to1(c), device_id_type=MESH), slot

    def rs2_copy(k, b, c, hop):
        slot = ((side - 1) * k + hop) % 2
        return pltpu.make_async_remote_copy(
            src_ref=s2.at[b, c], dst_ref=r2.at[b, c, slot],
            send_sem=s2_sem.at[b, c], recv_sem=r2_sem.at[b, c, slot],
            device_id=to2(c), device_id_type=MESH), slot

    def y_at(k, b, c, row, nrows, piece):
        return y_hbm.at[
            pl.ds(pl.multiple_of(k * chunk + b * rb + row, rs), nrows),
            pl.ds(pl.multiple_of((c * side + piece) * ct, ct), ct)]

    def ag2_copy(k, b, c, hop):
        ref = y_at(k, b, c, piece2(c, hop - 1) * rs, rs, piece1(c, -1))
        return pltpu.make_async_remote_copy(
            src_ref=s2.at[b, c] if hop == 0 else ref, dst_ref=ref,
            send_sem=g2_send.at[b, c], recv_sem=g2_recv.at[b, c, hop, k % 2],
            device_id=to2(c), device_id_type=MESH)

    def ag2_arrival(k, b, c, hop):
        ref = y_at(k, b, c, piece2(c, hop) * rs, rs, piece1(c, -1))
        return pltpu.make_async_remote_copy(
            src_ref=ref, dst_ref=ref,
            send_sem=g2_send.at[b, c], recv_sem=g2_recv.at[b, c, hop, k % 2],
            device_id=to2(c), device_id_type=MESH)

    def ag1_copy(k, b, c, hop):
        ref = y_at(k, b, c, 0, rb, piece1(c, hop - 1))
        return pltpu.make_async_remote_copy(
            src_ref=ref, dst_ref=ref,
            send_sem=g1_send.at[b, c], recv_sem=g1_recv.at[b, c, hop, k % 2],
            device_id=to1(c), device_id_type=MESH)

    def ag1_arrival(k, b, c, hop):
        ref = y_at(k, b, c, 0, rb, piece1(c, hop))
        return pltpu.make_async_remote_copy(
            src_ref=ref, dst_ref=ref,
            send_sem=g1_send.at[b, c], recv_sem=g1_recv.at[b, c, hop, k % 2],
            device_id=to1(c), device_id_type=MESH)

    def own_copy(k, b, c):
        return pltpu.make_async_copy(
            s2.at[b, c], y_at(k, b, c, piece2(c, -1) * rs, rs, piece1(c, -1)), own_sem.at[b, c])

    last = side - 1

    def event(e, k, b):
        half = pl.ds(pl.multiple_of(b * rb, rb), rb)
        for c in range(4):
            if e < last:
                copy, _ = rs1_copy(k, b, c, e)
                if e == 0:
                    s1[b, c] = t_v[c, e, half, :].astype(jnp.bfloat16)
                else:
                    prev, slot = rs1_copy(k, b, c, e - 1)
                    prev.wait_recv()
                    prev.wait_send()
                    s1[b, c] = (r1[b, c, slot].astype(jnp.float32) + t_v[c, e, half, :]).astype(jnp.bfloat16)

                    @pl.when((side - 1) * k + (e - 1) < (side - 1) * nk - 2)
                    def _():
                        pl.semaphore_signal(free1.at[b, c], inc=1, device_id=from1(c), device_id_type=MESH)

                @pl.when((side - 1) * k + e >= 2)
                def _():
                    pl.semaphore_wait(free1.at[b, c], 1)

                copy.start()
            elif e < 2 * last:
                f = e - last
                if f == 0:
                    prev, slot = rs1_copy(k, b, c, last - 1)
                    prev.wait_recv()
                    prev.wait_send()
                    t_v[c, last, half, :] = r1[b, c, slot].astype(jnp.float32) + t_v[c, last, half, :]

                    @pl.when((side - 1) * k + (last - 1) < (side - 1) * nk - 2)
                    def _():
                        pl.semaphore_signal(free1.at[b, c], inc=1, device_id=from1(c), device_id_type=MESH)

                part = pl.ds(pl.multiple_of(b * rb + piece2(c, f) * rs, rs), rs)
                if f == 0:
                    s2[b, c] = t_v[c, last, part, :].astype(jnp.bfloat16)
                else:
                    prev, slot = rs2_copy(k, b, c, f - 1)
                    prev.wait_recv()
                    prev.wait_send()
                    s2[b, c] = (r2[b, c, slot].astype(jnp.float32) + t_v[c, last, part, :]).astype(jnp.bfloat16)

                    @pl.when((side - 1) * k + (f - 1) < (side - 1) * nk - 2)
                    def _():
                        pl.semaphore_signal(free2.at[b, c], inc=1, device_id=from2(c), device_id_type=MESH)

                @pl.when((side - 1) * k + f >= 2)
                def _():
                    pl.semaphore_wait(free2.at[b, c], 1)

                copy, _ = rs2_copy(k, b, c, f)
                copy.start()
            elif e < 3 * last:
                f = e - 2 * last
                if f == 0:
                    part = pl.ds(pl.multiple_of(b * rb + piece2(c, last) * rs, rs), rs)
                    prev, slot = rs2_copy(k, b, c, last - 1)
                    prev.wait_recv()
                    prev.wait_send()
                    s2[b, c] = (r2[b, c, slot].astype(jnp.float32) + t_v[c, last, part, :]).astype(jnp.bfloat16)

                    @pl.when((side - 1) * k + (last - 1) < (side - 1) * nk - 2)
                    def _():
                        pl.semaphore_signal(free2.at[b, c], inc=1, device_id=from2(c), device_id_type=MESH)

                    own_copy(k, b, c).start()
                else:
                    ag2_arrival(k, b, c, f - 1).wait_recv()
                    ag2_copy(k, b, c, f - 1).wait_send()
                    if f == 1:
                        own_copy(k, b, c).wait()
                ag2_copy(k, b, c, f).start()
            elif e < 4 * last:
                f = e - 3 * last
                if f == 0:
                    ag2_arrival(k, b, c, last - 1).wait_recv()
                    ag2_copy(k, b, c, last - 1).wait_send()
                else:
                    ag1_arrival(k, b, c, f - 1).wait_recv()
                    ag1_copy(k, b, c, f - 1).wait_send()
                ag1_copy(k, b, c, f).start()
            else:
                ag1_arrival(k, b, c, last - 1).wait_recv()
                ag1_copy(k, b, c, last - 1).wait_send()

    def communicate(g):
        b = g % 2
        u = g // 2
        k1 = u // STEPS
        e1 = u % STEPS

        @pl.when((e1 == 0) & (k1 >= 2))
        def _():
            event(2 * STEPS, k1 - 2, b)

        for e in range(STEPS):
            @pl.when((e1 == e) & (k1 >= 1) & (k1 <= nk))
            def _():
                event(e + STEPS, k1 - 1, b)

            @pl.when((e1 == e) & (k1 < nk))
            def _():
                event(e, k1, b)

    x_copy(0).start()
    for copy in gate_copies(0):
        copy.start()

    @pl.loop(0, (nk + 2) * ticks)
    def _(n):
        k = n // ticks
        t = n % ticks
        q = t - gate_ticks

        @pl.when((k < nk) & (t < gate_ticks))
        def _():
            @pl.when(t == 0)
            def _():
                x_copy(k).wait()

            for copy in gate_copies(t):
                copy.wait()

            @pl.when(t + 1 < gate_ticks)
            def _():
                for copy in gate_copies(t + 1):
                    copy.start()

            @pl.when(t == gate_ticks - 2)
            def _():
                down_copy(0).start()

            s = t % 2
            for i in range(2):
                part = slice(i * chunk // 2, (i + 1) * chunk // 2)
                gate = jnp.dot(x_v[part, :], wg_v[s], preferred_element_type=jnp.float32)
                up = jnp.dot(x_v[part, :], wu_v[s], preferred_element_type=jnp.float32)
                h_v[part, pl.ds(pl.multiple_of(t * tn, tn), tn)] = (gate * jax.nn.sigmoid(gate) * up).astype(jnp.bfloat16)

        @pl.when((k < nk) & (t >= gate_ticks))
        def _():
            down_copy(q).wait()

            @pl.when(q + 1 < down_ticks)
            def _():
                down_copy(q + 1).start()

            @pl.when((q == 0) & (k + 1 < nk))
            def _():
                x_copy(k + 1).start()

            @pl.when((q == down_ticks // 2) & (k + 1 < nk))
            def _():
                for copy in gate_copies(0):
                    copy.start()

            for i in range(2):
                part = slice(i * chunk // 2, (i + 1) * chunk // 2)
                t_v[q % 4, q // 4, part, :] = jnp.dot(h_v[part, :], wd_v[q % 2], preferred_element_type=jnp.float32)

        @pl.when((k > 0) & (t < gate_ticks) & (t % 3 > 0))
        def _():
            communicate(2 * STEPS * (k - 1) + 4 + (t // 3) * 2 + t % 3 - 1)

        @pl.when((t >= gate_ticks) & (q % 4 == 3) & (2 * STEPS * k + q // 4 < 2 * STEPS * (nk + 1) + 2))
        def _():
            communicate(2 * STEPS * k + q // 4)


def solution(mesh):
    side = math.isqrt(mesh.shape["tp"])

    def step(x, w_gate, w_up, w_down):
        rows, d = x.shape
        f = w_gate.shape[1]
        chunk = min(CHUNK, rows)
        tn, ct, rb = f // GATE_TICKS, d // (4 * side), chunk // 2
        rs = rb // side
        bf16, f32 = jnp.bfloat16, jnp.float32
        dma = pltpu.SemaphoreType.DMA
        return pl.pallas_call(
            functools.partial(kernel, side, chunk),
            out_shape=jax.ShapeDtypeStruct((rows, d), bf16),
            in_specs=[pl.BlockSpec(memory_space=pl.ANY)] * 4,
            out_specs=pl.BlockSpec(memory_space=pl.ANY),
            scratch_shapes=[
                pltpu.VMEM((chunk, d), bf16),
                pltpu.VMEM((chunk, f), bf16),
                pltpu.VMEM((2, d, tn), bf16),
                pltpu.VMEM((2, d, tn), bf16),
                pltpu.VMEM((2, f, ct), bf16),
                pltpu.VMEM((4, side, chunk, ct), f32),
                pltpu.VMEM((2, 4, 2, rb, ct), bf16),
                pltpu.VMEM((2, 4, rb, ct), bf16),
                pltpu.VMEM((2, 4, 2, rs, ct), bf16),
                pltpu.VMEM((2, 4, rs, ct), bf16),
                dma, dma((2,)), dma((2,)), dma((2,)),
                dma((2, 4, 2)), dma((2, 4)), dma((2, 4, 2)), dma((2, 4)),
                dma((2, 4, side - 1, 2)), dma((2, 4)), dma((2, 4, side - 1, 2)), dma((2, 4)), dma((2, 4)),
                pltpu.SemaphoreType.REGULAR((2, 4)), pltpu.SemaphoreType.REGULAR((2, 4)),
            ],
            compiler_params=pltpu.CompilerParams(
                collective_id=0, has_side_effects=True, vmem_limit_bytes=67043328),
        )(x, w_gate, w_up, w_down)

    return jax.shard_map(
        step,
        mesh=mesh,
        in_specs=(P("dp", None), P(None, "tp"), P(None, "tp"), P("tp", None)),
        out_specs=P("dp", None),
        check_vma=False,
    )
```
